16 devices in a mesh: dp: 4 (over z, y), tp: 4 (over x, core).
Axes of the slice: x: 2, y: 2, z: 2, core: 2. Of those that a mesh axis runs over, the one named last changes fastest.
Arguments:
- x_norm: bfloat16 [8192, 2048], P(('dp', 'tp')), parts along dimension 0
- grad_y: bfloat16 [8192, 2048], P(('dp', 'tp')), parts along dimension 0
- u_gate: bfloat16 [8192, 8192], P('dp', 'tp'), parts along dimension 0
- u_up: bfloat16 [8192, 8192], P('dp', 'tp'), parts along dimension 0
- w_gate: bfloat16 [2048, 8192], P(None, 'tp')
- w_up: bfloat16 [2048, 8192], P(None, 'tp')
- w_down: bfloat16 [8192, 2048], P('tp')
- x_in: bfloat16 [8192, 2048], P(('dp', 'tp')), parts along dimension 0
- gamma: bfloat16 [2048], replicated
- grad_res: bfloat16 [8192, 2048], P(('dp', 'tp')), parts along dimension 0
- attn_out: bfloat16 [8192, 2048], P('dp', 'tp'), parts along dimension 0
- w_out: bfloat16 [2048, 2048], P('tp')
Outputs:
- output 1: bfloat16 [8192, 2048], P(('dp', 'tp')), parts along dimension 0
- output 2: bfloat16 [8192, 2048], P('dp', 'tp'), parts along dimension 0
- output 3: float32 [8192, 8192], P('dp', 'tp'), parts along dimension 0
- output 4: float32 [8192, 8192], P('dp', 'tp'), parts along dimension 0
- output 5: float32 [32768, 2048], P(('dp', 'tp')), parts along dimension 0
- output 6: float32 [8192, 2048], P(('dp', 'tp')), parts along dimension 0
There are 4 independent parts. The reference program is written for one: setup_inputs(seed, part) draws one part's arguments, and reference() takes and returns one part's arrays. A program takes and returns all parts, laid end to end along the dimension named above; an argument that names none is the same for every part.
All inputs are finite; a program needn't handle non-finite values.
Results may differ from the reference program's by a relative error of at most 0.0124612.
Values are sent between devices in bfloat16 or wider.
A program may use at most 1 GiB of HBM per device.

```python
import jax
import jax.numpy as jnp
from jax import lax

HIDDEN = 2048
FFN_DIM = 8192
TOKENS = 2048
NORM_EPS = 1e-5


def setup_inputs(seed: int = 0, part: int = 0) -> dict:
    part_keys = jax.random.split(jax.random.fold_in(jax.random.key(seed), part), 7)
    weight_keys = jax.random.split(jax.random.key(seed + 1), 5)
    xin_keys = jax.random.split(part_keys[4], 2)
    act_shape = (TOKENS, HIDDEN)
    ffn_shape = (TOKENS, FFN_DIM)
    x_norm = jax.random.normal(part_keys[0], act_shape, jnp.float32)
    grad_y = jax.random.normal(part_keys[1], act_shape, jnp.float32)
    u_gate = jax.random.normal(part_keys[2], ffn_shape, jnp.float32)
    u_up = jax.random.normal(part_keys[3], ffn_shape, jnp.float32)
    xin_scale = jnp.exp(jax.random.uniform(xin_keys[0], (TOKENS, 1), jnp.float32, -1.0, 1.0))
    x_in = jax.random.normal(xin_keys[1], act_shape, jnp.float32) * xin_scale
    grad_res = 0.5 * jax.random.normal(part_keys[5], act_shape, jnp.float32)
    attn_out = jax.random.normal(part_keys[6], act_shape, jnp.float32)
    w_gate = jax.random.normal(weight_keys[0], (HIDDEN, FFN_DIM), jnp.float32) * HIDDEN ** -0.5
    w_up = jax.random.normal(weight_keys[1], (HIDDEN, FFN_DIM), jnp.float32) * HIDDEN ** -0.5
    w_down = jax.random.normal(weight_keys[2], (FFN_DIM, HIDDEN), jnp.float32) * FFN_DIM ** -0.5
    w_out = jax.random.normal(weight_keys[3], (HIDDEN, HIDDEN), jnp.float32) * HIDDEN ** -0.5
    gamma = 1.0 + 0.3 * jax.random.normal(weight_keys[4], (HIDDEN,), jnp.float32)
    return dict(
        x_norm=x_norm.astype(jnp.bfloat16),
        grad_y=grad_y.astype(jnp.bfloat16),
        u_gate=u_gate.astype(jnp.bfloat16),
        u_up=u_up.astype(jnp.bfloat16),
        w_gate=w_gate.astype(jnp.bfloat16),
        w_up=w_up.astype(jnp.bfloat16),
        w_down=w_down.astype(jnp.bfloat16),
        x_in=x_in.astype(jnp.bfloat16),
        gamma=gamma.astype(jnp.bfloat16),
        grad_res=grad_res.astype(jnp.bfloat16),
        attn_out=attn_out.astype(jnp.bfloat16),
        w_out=w_out.astype(jnp.bfloat16),
    )


def reference(x_norm, grad_y, u_gate, u_up, w_gate, w_up, w_down, x_in, gamma, grad_res, attn_out, w_out):
    gate_f = u_gate.astype(jnp.float32)
    up_f = u_up.astype(jnp.float32)
    sig_gate = jax.nn.sigmoid(gate_f)
    act_gate = gate_f * sig_gate
    silu_grad = sig_gate * (1.0 + gate_f * (1.0 - sig_gate))
    hidden_z = (act_gate * up_f).astype(jnp.bfloat16)
    gw_down = jnp.dot(hidden_z.T, grad_y, preferred_element_type=jnp.float32)
    grad_h = jnp.dot(grad_y, w_down.T, preferred_element_type=jnp.float32)
    grad_up = (grad_h * act_gate).astype(jnp.bfloat16)
    grad_gate = (grad_h * up_f * silu_grad).astype(jnp.bfloat16)
    grad_x = (jnp.dot(grad_gate, w_gate.T, preferred_element_type=jnp.float32)
              + jnp.dot(grad_up, w_up.T, preferred_element_type=jnp.float32)).astype(jnp.bfloat16)
    gw_gate = jnp.dot(x_norm.T, grad_gate, preferred_element_type=jnp.float32)
    gw_up = jnp.dot(x_norm.T, grad_up, preferred_element_type=jnp.float32)
    xin_f = x_in.astype(jnp.float32)
    inv_rms = lax.rsqrt(jnp.mean(xin_f * xin_f, axis=-1, keepdims=True) + NORM_EPS)
    scaled = grad_x.astype(jnp.float32) * gamma.astype(jnp.float32)
    proj_mean = jnp.mean(scaled * xin_f, axis=-1, keepdims=True)
    grad_sum = (grad_res.astype(jnp.float32)
                + inv_rms * (scaled - xin_f * (inv_rms * inv_rms) * proj_mean)).astype(jnp.bfloat16)
    grad_attn = jnp.dot(grad_sum, w_out.T, preferred_element_type=jnp.float32).astype(jnp.bfloat16)
    gw_out = jnp.dot(attn_out.T, grad_sum, preferred_element_type=jnp.float32)
    return grad_sum, grad_attn, gw_gate, gw_up, gw_down, gw_out
```

```python
import functools

import jax
import jax.numpy as jnp
from jax import lax
from jax.experimental import pallas as pl
from jax.experimental.pallas import tpu as pltpu
from jax.sharding import PartitionSpec as P


F32 = jnp.float32
BF16 = jnp.bfloat16
NORM_EPS = 1e-5
ROWS_T = (((0,), (0,)), ((), ()))
COLS_T = (((1,), (1,)), ((), ()))
ANY = pl.BlockSpec(memory_space=pl.ANY)
VMEM_LIMIT = 60 * 1024 * 1024
BLOCK = 512

CROSS = [(0, 2), (2, 0), (1, 3), (3, 1)]
PAIR = [(0, 1), (1, 0), (2, 3), (3, 2)]
OWN, SIB, FAR, DIAG = 0, 1, 2, 3


def dot(a, b, dims):
    return lax.dot_general(a, b, dims, preferred_element_type=F32)


def block_of(k):
    return lax.axis_index("tp") ^ k


def params(limit=VMEM_LIMIT):
    return pltpu.CompilerParams(vmem_limit_bytes=limit)


def hbm(*arrays):
    return [pltpu.with_memory_space_constraint(a, pltpu.HBM) for a in arrays]


def once(shape, index=None):
    return pl.BlockSpec(shape, index or (lambda *_: (0,) * len(shape)), pipeline_mode=pl.Buffered(1))


def hidden_body(n, tiles, *refs):
    dys, ugs, uus = refs[:n], refs[n:2 * n], refs[2 * n:3 * n]
    wd, wg, wu = refs[3 * n:3 * n + 3]
    dg, du, z = refs[-(n + 6):-(n + 3)]
    ps, (acc, held_g, held_u) = refs[-(n + 3):-3], refs[-3:]
    step = pl.program_id(0)
    rows = dys[0].shape[0]

    def form(slot):
        for i in range(n):
            span = pl.ds(i * rows, rows)
            grad_h = dot(dys[i][...], wd[...], COLS_T)
            gate = ugs[i][...].astype(F32)
            up = uus[i][...].astype(F32)
            sig = jax.nn.sigmoid(gate)
            act = gate * sig
            z[span, :] = (act * up).astype(BF16)
            grad_up = (grad_h * act).astype(BF16)
            grad_gate = (grad_h * up * (sig * (1.0 + gate * (1.0 - sig)))).astype(BF16)
            du[span, :] = grad_up
            dg[span, :] = grad_gate
            held_u[slot, span, :] = grad_up
            held_g[slot, span, :] = grad_gate

    def term(slot):
        return dot(held_g[slot], wg[...], COLS_T) + dot(held_u[slot], wu[...], COLS_T)

    @pl.when(step == 0)
    def _():
        acc[...] = jnp.zeros_like(acc)
        form(0)

    @pl.when((step > 0) & (step < tiles))
    def _():
        slot = lax.rem(step, 2)
        acc[...] += term(1 - slot)
        form(slot)

    @pl.when(step == tiles)
    def _():
        total = acc[...] + term((tiles - 1) % 2)
        for i in range(n):
            ps[i][...] = total[i * rows:(i + 1) * rows].astype(BF16)


def hidden(blocks, dys, start, rows, u_gate, u_up, w_down, w_gate, w_up, deps=(), tile=512):
    n = len(blocks)
    width = dys[0].shape[1]
    cols = w_down.shape[0]
    tiles = cols // tile
    per, first = BLOCK // rows, start // rows
    now = lambda s: jnp.minimum(s, tiles - 1)
    before = lambda s: jnp.maximum(s - 1, 0)
    u_specs = [pl.BlockSpec((rows, tile), functools.partial(lambda k, s: (block_of(k) * per + first, now(s)), k)) for k in blocks]
    tile_out = pl.BlockSpec((n * rows, tile), lambda s: (0, now(s)))
    w_late = pl.BlockSpec((width, tile), lambda s: (0, before(s)))
    return pl.pallas_call(
        functools.partial(hidden_body, n, tiles),
        grid=(tiles + 1,),
        in_specs=[once((rows, width), lambda s: (first, 0))] * n + u_specs + u_specs
        + [pl.BlockSpec((tile, width), lambda s: (now(s), 0)), w_late, w_late] + [ANY] * len(deps),
        out_specs=[tile_out] * 3 + [once((rows, width))] * n,
        out_shape=[jax.ShapeDtypeStruct((n * rows, cols), BF16)] * 3 + [jax.ShapeDtypeStruct((rows, width), BF16)] * n,
        scratch_shapes=[pltpu.VMEM((n * rows, width), F32)] + [pltpu.VMEM((2, n * rows, tile), BF16)] * 2,
        compiler_params=params(),
        cost_estimate=pl.CostEstimate(flops=6 * n * rows * width * cols, bytes_accessed=50 << 20, transcendentals=n * rows * cols),
    )(*hbm(*dys, *([u_gate] * n), *([u_up] * n), w_down, w_gate, w_up, *deps))


def grad_body(n, *refs):
    lefts, rights, out = refs[:n], refs[n:2 * n], refs[-1]
    total = dot(lefts[0][...], rights[0][...], ROWS_T)
    for a, b in zip(lefts[1:], rights[1:]):
        total += dot(a[...], b[...], ROWS_T)
    out[...] = total


def weight_grad(lefts, rights, deps=(), tm=256, tn=2048):
    n = len(lefts)
    m, cols = lefts[0][0].shape[1], rights[0][0].shape[1]
    l_specs = [pl.BlockSpec((r, tm), functools.partial(lambda b, j, i: (b, i), s // r)) for _, s, r in lefts]
    r_specs = [(pl.BlockSpec if tn < cols else once)((r, tn), functools.partial(lambda b, j, i: (b, j), s // r)) for _, s, r in rights]
    tokens = sum(r for _, _, r in lefts)
    return pl.pallas_call(
        functools.partial(grad_body, n),
        grid=(cols // tn, m // tm),
        in_specs=l_specs + r_specs + [ANY] * len(deps),
        out_specs=pl.BlockSpec((tm, tn), lambda j, i: (i, j)),
        out_shape=jax.ShapeDtypeStruct((m, cols), F32),
        compiler_params=params(),
        cost_estimate=pl.CostEstimate(flops=2 * tokens * m * cols, bytes_accessed=32 << 20, transcendentals=0),
    )(*hbm(*[a for a, _, _ in lefts], *[a for a, _, _ in rights], *deps))


def add_body(a, b, *refs):
    refs[-1][...] = (a[...].astype(F32) + b[...].astype(F32)).astype(BF16)


def add(a, b, tile=64):
    rows, width = a.shape
    spec = pl.BlockSpec((tile, width), lambda i: (i, 0))
    return pl.pallas_call(
        add_body,
        grid=(rows // tile,),
        in_specs=[spec, spec],
        out_specs=spec,
        out_shape=jax.ShapeDtypeStruct((rows, width), BF16),
        compiler_params=params(24 << 20),
        cost_estimate=pl.CostEstimate(flops=1000 * rows * width, bytes_accessed=6 * rows * width, transcendentals=0),
    )(*hbm(a, b))


def norm_body(p_own, p_pair, p_far, x_in, grad_res, gamma, *refs):
    piece, whole = refs[-2:]
    grad_x = (p_own[...].astype(F32) + p_pair[...].astype(F32) + p_far[...].astype(F32)).astype(BF16)
    xin = x_in[...].astype(F32)
    inv = lax.rsqrt(jnp.mean(xin * xin, axis=-1, keepdims=True) + NORM_EPS)
    scaled = grad_x.astype(F32) * gamma[...].astype(F32)
    proj = jnp.mean(scaled * xin, axis=-1, keepdims=True)
    res = (grad_res[...].astype(F32) + inv * (scaled - xin * (inv * inv) * proj)).astype(BF16)
    piece[...] = res
    whole[...] = res


def norm_backward(start, p_own, p_pair, p_far, x_in, grad_res, gamma, prev, deps=(), tile=64):
    rows, width = p_far.shape
    first = start // tile
    here = pl.BlockSpec((tile, width), lambda i: (first + i, 0))
    part = pl.BlockSpec((tile, width), lambda i: (i, 0))
    extra = ([] if prev is None else [prev]) + list(deps)
    return pl.pallas_call(
        norm_body,
        grid=(rows // tile,),
        in_specs=[here, here, part, here, here, once((1, width))] + [ANY] * len(extra),
        out_specs=[part, here],
        out_shape=[jax.ShapeDtypeStruct((rows, width), BF16), jax.ShapeDtypeStruct(p_own.shape, BF16)],
        input_output_aliases={} if prev is None else {6: 1},
        compiler_params=params(24 << 20),
        cost_estimate=pl.CostEstimate(flops=2000 * rows * width, bytes_accessed=14 * rows * width, transcendentals=0),
    )(*hbm(p_own, p_pair, p_far, x_in, grad_res, gamma, *extra))


def proj_body(blocks, start, first, *refs):
    ds0, ds1, o0, o1, w_out = refs[:5]
    prev_w = None if first else refs[5]
    grad_o, grad_w, acc, stage, sem = refs[-5:]
    step = pl.program_id(0)
    rows = ds0.shape[0]

    @pl.when(step == 0)
    def _():
        acc[...] = jnp.zeros_like(acc)

    acc[pl.ds(0, rows), :] += dot(ds0[...], w_out[...], COLS_T)
    acc[pl.ds(rows, rows), :] += dot(ds1[...], w_out[...], COLS_T)
    total = dot(o0[...], ds0[...], ROWS_T) + dot(o1[...], ds1[...], ROWS_T)
    grad_w[...] = total if first else prev_w[...] + total

    @pl.when(step == pl.num_programs(0) - 1)
    def _():
        stage[...] = acc[...].astype(BF16)
        copies = [
            pltpu.make_async_copy(
                stage.at[pl.ds(i * rows, rows), :],
                grad_o.at[pl.ds(pl.multiple_of(block_of(k) * BLOCK + start, rows), rows), :],
                sem.at[i])
            for i, k in enumerate(blocks)
        ]
        for c in copies:
            c.start()
        for c in copies:
            c.wait()


def out_proj(blocks, start, ds0, ds1, attn_out, w_out, prev, deps=(), tile=512):
    rows, width = ds0.shape
    tokens, cols = attn_out.shape
    per = BLOCK // rows
    o_specs = [pl.BlockSpec((rows, cols), functools.partial(lambda k, h: (block_of(k) * per + start // rows, 0), k),
                            pipeline_mode=pl.Buffered(1)) for k in blocks]
    w_spec = pl.BlockSpec((cols, tile), lambda h: (0, h))
    first = prev is None
    return pl.pallas_call(
        functools.partial(proj_body, blocks, start, first),
        grid=(width // tile,),
        in_specs=[pl.BlockSpec((rows, tile), lambda h: (0, h))] * 2 + o_specs + [w_spec]
        + ([] if first else [w_spec, ANY]) + [ANY] * len(deps),
        out_specs=[ANY, w_spec],
        out_shape=[jax.ShapeDtypeStruct((tokens, cols), BF16), jax.ShapeDtypeStruct((cols, width), F32)],
        scratch_shapes=[pltpu.VMEM((2 * rows, cols), F32), pltpu.VMEM((2 * rows, cols), BF16), pltpu.SemaphoreType.DMA((2,))],
        input_output_aliases={} if first else {5: 1, 6: 0},
        compiler_params=params(24 << 20),
        cost_estimate=pl.CostEstimate(flops=8 * rows * width * cols, bytes_accessed=8 << 20, transcendentals=0),
    )(*hbm(ds0, ds1, attn_out, attn_out, w_out, *([] if first else [prev[1], prev[0]]), *deps))


CHUNK = 256


def solution(mesh):
    token_spec = P(("dp", "tp"), None)
    split_cols = P("dp", "tp")
    weight_cols = P(None, "tp")
    weight_rows = P("tp", None)

    def cross(a):
        return lax.ppermute(a, "tp", CROSS)

    def pair(a):
        return lax.ppermute(a, "tp", PAIR)

    def after(a, *others):
        return lax.optimization_barrier((a,) + others)[0]

    def body(x_norm, grad_y, u_gate, u_up, w_gate, w_up, w_down, x_in, gamma, grad_res, attn_out, w_out):
        gamma = gamma.reshape(1, -1)
        gy_far = cross(grad_y)
        gy_sib = pair(grad_y)
        x_far = cross(x_norm)
        x_sib = pair(x_norm)
        starts = range(0, BLOCK, CHUNK)

        args = (u_gate, u_up, w_down, w_gate, w_up)
        dg_near, du_near, z_near, p_own, p_sib = hidden((OWN, SIB), (grad_y, gy_sib), 0, BLOCK, *args)
        p_pair = pair(p_sib)
        gy_far = after(gy_far, p_own)
        gy_diag = pair(gy_far)
        dgs, dus, zs, sends, deps = [], [], [], [], ()
        for at in starts:
            dg, du, z, p_far, p_diag = hidden((FAR, DIAG), (gy_far, gy_diag), at, CHUNK, *args, deps=deps)
            p_sum = add(p_far, pair(p_diag))
            dgs.append(dg), dus.append(du), zs.append(z), sends.append(p_sum)
            deps = (p_sum,)
        recvs = [cross(s) for s in sends]

        def pieces(own, sib, far, diag):
            return [(own, 0, BLOCK), (sib, 0, BLOCK)] + [(a, at, CHUNK) for at in starts for a in (far, diag)]

        def stacked(near, fars):
            return [(near, 0, BLOCK), (near, BLOCK, BLOCK)] + [(a, at, CHUNK) for a in fars for at in (0, CHUNK)]

        x_far = after(x_far, sends[-1])
        x_diag = pair(x_far)
        gw_down = weight_grad(stacked(z_near, zs), pieces(grad_y, gy_sib, gy_far, gy_diag), deps=(sends[-1],))
        xs = pieces(x_norm, x_sib, x_far, x_diag)

        whole, fars, prev = None, [], gw_down
        grads = []
        for c, at in enumerate(starts):
            piece, whole = norm_backward(at, p_own, p_pair, after(recvs[c], prev), x_in, grad_res, gamma, whole)
            fars.append(cross(piece))
            rights = stacked(*((dg_near, dgs), (du_near, dus))[c])
            prev = weight_grad(xs, rights, deps=(piece,))
            grads.append(prev)
        sib = pair(whole)
        res = out_proj((OWN, SIB), 0, whole, sib, attn_out, w_out, None, deps=(grads[1],))
        for c, at in enumerate(starts):
            far = after(fars[c], res[1])
            res = out_proj((FAR, DIAG), at, far, pair(far), attn_out, w_out, res)
        grad_attn, gw_out = res
        return whole, grad_attn, grads[0], grads[1], gw_down, gw_out


    return jax.shard_map(
        body,
        mesh=mesh,
        in_specs=(token_spec, token_spec, split_cols, split_cols, weight_cols, weight_cols, weight_rows,
                  token_spec, P(None), token_spec, split_cols, weight_rows),
        out_specs=(token_spec, split_cols, split_cols, split_cols, token_spec, token_spec),
        check_vma=False,
    )
```

```python
import functools

import jax
import jax.numpy as jnp
from jax import lax
from jax.experimental import pallas as pl
from jax.experimental.pallas import tpu as pltpu
from jax.sharding import PartitionSpec as P


F32 = jnp.float32
BF16 = jnp.bfloat16
NORM_EPS = 1e-5
ROWS_T = (((0,), (0,)), ((), ()))
COLS_T = (((1,), (1,)), ((), ()))
ANY = pl.BlockSpec(memory_space=pl.ANY)
VMEM_LIMIT = 60 * 1024 * 1024
ALL_VMEM = 67043328
BLOCK = 512

CROSS = [(0, 2), (2, 0), (1, 3), (3, 1)]
PAIR = [(0, 1), (1, 0), (2, 3), (3, 2)]
OWN, SIB, FAR, DIAG = 0, 1, 2, 3


def dot(a, b, dims):
    return lax.dot_general(a, b, dims, preferred_element_type=F32)


def block_of(k):
    return lax.axis_index("tp") ^ k


def params(limit=VMEM_LIMIT):
    return pltpu.CompilerParams(vmem_limit_bytes=limit)


def hbm(*arrays):
    return [pltpu.with_memory_space_constraint(a, pltpu.HBM) for a in arrays]


def once(shape, index=None):
    return pl.BlockSpec(shape, index or (lambda *_: (0,) * len(shape)), pipeline_mode=pl.Buffered(1))


def hidden_body(n, tiles, parts, down, *refs):
    dys, ugs, uus = refs[:n], refs[n:2 * n], refs[2 * n:3 * n]
    wd, wg, wu = refs[3 * n:3 * n + 3]
    m = n * parts
    outs = refs[-(m + 5 + (down > 0) + (down < n)):-(m + 3)]
    dg, du = outs[:2]
    ps, (acc, held_g, held_u) = refs[-(m + 3):-3], refs[-3:]
    step = pl.program_id(0)
    rows = dys[0].shape[0]
    piece = rows // parts

    def form(slot):
        total = None
        for i in range(n):
            span = pl.ds(i * rows, rows)
            grad_h = dot(dys[i][...], wd[...], COLS_T)
            gate = ugs[i][...].astype(F32)
            up = uus[i][...].astype(F32)
            sig = jax.nn.sigmoid(gate)
            act = gate * sig
            hidden_z = (act * up).astype(BF16)
            grad_up = (grad_h * act).astype(BF16)
            grad_gate = (grad_h * up * (sig * (1.0 + gate * (1.0 - sig)))).astype(BF16)
            du[span, :] = grad_up
            dg[span, :] = grad_gate
            held_u[slot, span, :] = grad_up
            held_g[slot, span, :] = grad_gate
            if i < down:
                more = dot(hidden_z, dys[i][...], ROWS_T)
                total = more if total is None else total + more
            else:
                outs[-1][pl.ds((i - down) * rows, rows), :] = hidden_z
        if down:
            outs[2][...] = total

    def term(slot):
        return dot(held_g[slot], wg[...], COLS_T) + dot(held_u[slot], wu[...], COLS_T)

    @pl.when(step == 0)
    def _():
        form(0)

    @pl.when((step > 0) & (step < tiles))
    def _():
        slot = lax.rem(step, 2)
        acc[...] = jnp.where(step == 1, 0.0, acc[...]) + term(1 - slot)
        form(slot)

    @pl.when(step == tiles)
    def _():
        total = acc[...] + term((tiles - 1) % 2)
        for i in range(m):
            ps[i][...] = total[i * piece:(i + 1) * piece].astype(BF16)


def hidden(blocks, dys, parts, down, u_gate, u_up, w_down, w_gate, w_up, deps=(), tile=512):
    n = len(blocks)
    rows, width = dys[0].shape
    cols = w_down.shape[0]
    tiles = cols // tile
    now = lambda s: jnp.minimum(s, tiles - 1)
    before = lambda s: jnp.maximum(s - 1, 0)
    u_specs = [pl.BlockSpec((rows, tile), functools.partial(lambda k, s: (block_of(k), now(s)), k)) for k in blocks]
    tile_out = pl.BlockSpec((n * rows, tile), lambda s: (0, now(s)))
    z_out = pl.BlockSpec(((n - down) * rows, tile), lambda s: (0, now(s)))
    w_late = pl.BlockSpec((width, tile), lambda s: (0, before(s)))
    w_now = pl.BlockSpec((tile, width), lambda s: (now(s), 0))
    wide = jax.ShapeDtypeStruct((n * rows, cols), BF16)
    piece = (rows // parts, width)
    return pl.pallas_call(
        functools.partial(hidden_body, n, tiles, parts, down),
        grid=(tiles + 1,),
        in_specs=[once((rows, width))] * n + u_specs + u_specs + [w_now, w_late, w_late] + [ANY] * len(deps),
        out_specs=[tile_out] * 2 + [w_now] * (down > 0) + [z_out] * (down < n) + [once(piece)] * (n * parts),
        out_shape=[wide] * 2 + [jax.ShapeDtypeStruct((cols, width), F32)] * (down > 0)
        + [jax.ShapeDtypeStruct(((n - down) * rows, cols), BF16)] * (down < n)
        + [jax.ShapeDtypeStruct(piece, BF16)] * (n * parts),
        scratch_shapes=[pltpu.VMEM((n * rows, width), F32)] + [pltpu.VMEM((2, n * rows, tile), BF16)] * 2,
        compiler_params=params(),
        cost_estimate=pl.CostEstimate(flops=(6 * n + 2 * down) * rows * width * cols, bytes_accessed=50 << 20,
                                      transcendentals=n * rows * cols),
    )(*dys, *hbm(*([u_gate] * n), *([u_up] * n), w_down, w_gate, w_up, *deps))


def grad_body(n, *refs):
    lefts, rights, out = refs[:n], refs[n:2 * n], refs[-1]
    total = dot(lefts[0][...], rights[0][...], ROWS_T)
    for a, b in zip(lefts[1:], rights[1:]):
        total += dot(a[...], b[...], ROWS_T)
    out[...] = total


def grad_more_body(n, *refs):
    lefts, rights, prev, out = refs[:n], refs[n:2 * n], refs[2 * n], refs[-1]
    total = prev[...]
    for a, b in zip(lefts, rights):
        total += dot(a[...], b[...], ROWS_T)
    out[...] = total


def weight_grad(lefts, rights, prev=None, deps=(), tm=256):
    n = len(lefts)
    m, cols = lefts[0][0].shape[1], rights[0][0].shape[1]
    l_specs = [pl.BlockSpec((BLOCK, tm), functools.partial(lambda b, i: (b, i), b)) for _, b in lefts]
    r_specs = [once((BLOCK, cols), functools.partial(lambda b, i: (b, 0), b)) for _, b in rights]
    out_spec = pl.BlockSpec((tm, cols), lambda i: (i, 0))
    more = [] if prev is None else [prev]
    return pl.pallas_call(
        functools.partial(grad_body if prev is None else grad_more_body, n),
        grid=(m // tm,),
        in_specs=l_specs + r_specs + [out_spec] * len(more) + [ANY] * len(deps),
        out_specs=out_spec,
        out_shape=jax.ShapeDtypeStruct((m, cols), F32),
        input_output_aliases={2 * n: 0} if more else {},
        compiler_params=params(),
        cost_estimate=pl.CostEstimate(flops=2 * n * BLOCK * m * cols, bytes_accessed=32 << 20, transcendentals=0),
    )(*hbm(*[a for a, _ in lefts], *[a for a, _ in rights], *more, *deps))


def spacer_body(*refs):
    refs[-1][...] = jnp.zeros_like(refs[-1])


def spacer(*deps):
    return pl.pallas_call(
        spacer_body,
        in_specs=[ANY] * len(deps),
        out_shape=jax.ShapeDtypeStruct((8, 128), F32),
        compiler_params=params(ALL_VMEM),
        cost_estimate=pl.CostEstimate(flops=1000, bytes_accessed=4096, transcendentals=0),
    )(*hbm(*deps))


def add_body(a, b, *refs):
    refs[-1][...] = (a[...].astype(F32) + b[...].astype(F32)).astype(BF16)


def add(a, b, tile=128):
    rows, width = a.shape
    spec = pl.BlockSpec((tile, width), lambda i: (i, 0))
    return pl.pallas_call(
        add_body,
        grid=(rows // tile,),
        in_specs=[spec, spec],
        out_specs=spec,
        out_shape=jax.ShapeDtypeStruct((rows, width), BF16),
        compiler_params=params(24 << 20),
        cost_estimate=pl.CostEstimate(flops=1000 * rows * width, bytes_accessed=6 * rows * width, transcendentals=0),
    )(*hbm(a), b)


def norm_body(p_own, p_pair, p_far, x_in, grad_res, gamma, *refs):
    piece, whole = refs[-2:]
    grad_x = (p_own[...].astype(F32) + p_pair[...].astype(F32) + p_far[...].astype(F32)).astype(BF16)
    xin = x_in[...].astype(F32)
    inv = lax.rsqrt(jnp.mean(xin * xin, axis=-1, keepdims=True) + NORM_EPS)
    scaled = grad_x.astype(F32) * gamma[...].astype(F32)
    proj = jnp.mean(scaled * xin, axis=-1, keepdims=True)
    res = (grad_res[...].astype(F32) + inv * (scaled - xin * (inv * inv) * proj)).astype(BF16)
    piece[...] = res
    whole[...] = res


def norm_backward(start, rows, p_own, p_pair, p_far, far_start, x_in, grad_res, gamma, prev, deps=(), tile=128):
    width = p_far.shape[1]
    first, far_first = start // tile, far_start // tile
    here = pl.BlockSpec((tile, width), lambda i: (first + i, 0))
    recv = pl.BlockSpec((tile, width), lambda i: (far_first + i, 0))
    part = pl.BlockSpec((tile, width), lambda i: (i, 0))
    extra = ([] if prev is None else [prev]) + list(deps)
    return pl.pallas_call(
        norm_body,
        grid=(rows // tile,),
        in_specs=[here, here, recv, here, here, once((1, width))] + [ANY] * len(extra),
        out_specs=[part, here],
        out_shape=[jax.ShapeDtypeStruct((rows, width), BF16), jax.ShapeDtypeStruct(p_own.shape, BF16)],
        input_output_aliases={} if prev is None else {6: 1},
        compiler_params=params(24 << 20),
        cost_estimate=pl.CostEstimate(flops=2000 * rows * width, bytes_accessed=14 * rows * width, transcendentals=0),
    )(*hbm(p_own, p_pair), p_far, *hbm(x_in, grad_res, gamma, *extra))


def proj_body(places, first, *refs):
    n = len(places)
    ds, o, w_out = refs[:n], refs[n:2 * n], refs[2 * n]
    grad_o, grad_w, acc, stage, sem = refs[-5:]
    step = pl.program_id(0)
    spans, at = [], 0
    for r in ds:
        spans.append(pl.ds(at, r.shape[0]))
        at += r.shape[0]

    @pl.when(step == 0)
    def _():
        acc[...] = jnp.zeros_like(acc)

    total = dot(o[0][...], ds[0][...], ROWS_T)
    for i in range(n):
        acc[spans[i], :] += dot(ds[i][...], w_out[...], COLS_T)
        if i:
            total += dot(o[i][...], ds[i][...], ROWS_T)
    grad_w[...] = total if first else refs[2 * n + 1][...] + total

    @pl.when(step == pl.num_programs(0) - 1)
    def _():
        stage[...] = acc[...].astype(BF16)
        copies = []
        for i, (k, start) in enumerate(places):
            rows = ds[i].shape[0]
            to = pl.ds(pl.multiple_of(block_of(k) * BLOCK + start, rows), rows)
            copies.append(pltpu.make_async_copy(stage.at[spans[i], :], grad_o.at[to, :], sem.at[i]))
        for c in copies:
            c.start()
        for c in copies:
            c.wait()


def out_proj(pieces, attn_out, w_out, prev, deps=(), tile=512):
    n = len(pieces)
    tokens, cols = attn_out.shape
    width = w_out.shape[1]
    sizes = [a.shape[0] for a, _, _ in pieces]
    places = [(k, start) for _, k, start in pieces]
    o_specs = [once((r, cols), functools.partial(lambda k, r, start, h: ((block_of(k) * BLOCK + start) // r, 0), k, r, start))
               for r, (k, start) in zip(sizes, places)]
    w_spec = pl.BlockSpec((cols, tile), lambda h: (0, h))
    first = prev is None
    return pl.pallas_call(
        functools.partial(proj_body, places, first),
        grid=(width // tile,),
        in_specs=[pl.BlockSpec((r, tile), lambda h: (0, h)) for r in sizes] + o_specs + [w_spec]
        + ([] if first else [w_spec, ANY]) + [ANY] * len(deps),
        out_specs=[ANY, w_spec],
        out_shape=[jax.ShapeDtypeStruct((tokens, cols), BF16), jax.ShapeDtypeStruct((cols, width), F32)],
        scratch_shapes=[pltpu.VMEM((sum(sizes), cols), F32), pltpu.VMEM((sum(sizes), cols), BF16), pltpu.SemaphoreType.DMA((n,))],
        input_output_aliases={} if first else {2 * n + 1: 1, 2 * n + 2: 0},
        compiler_params=params(24 << 20),
        cost_estimate=pl.CostEstimate(flops=4 * sum(sizes) * width * cols, bytes_accessed=8 << 20, transcendentals=0),
    )(*[a for a, _, _ in pieces], *hbm(*[attn_out] * n, w_out, *([] if first else [prev[1], prev[0]]), *deps))


def last_body(places, tile, *refs):
    n = len(places)
    ds, (o, w_out, prev_w) = refs[:n], refs[n:n + 3]
    grad_o, grad_w, held, stage, sem_w, sem_o = refs[-6:]
    rows = ds[0].shape[0]
    tiles = w_out.shape[1] // tile
    o_rows = [pl.ds(pl.multiple_of(block_of(k) * BLOCK + start, rows), rows) for k, start in places]

    def w_copy(h):
        cols = pl.ds(pl.multiple_of(h * tile, tile), tile)
        return pltpu.make_async_copy(held.at[:, cols], grad_w.at[:, cols], sem_w.at[h])

    def o_copy(i):
        return pltpu.make_async_copy(stage.at[pl.ds(i * rows, rows), :], grad_o.at[o_rows[i], :], sem_o.at[i])

    @pl.loop(0, tiles)
    def _(h):
        cols = pl.ds(pl.multiple_of(h * tile, tile), tile)
        total = dot(o[o_rows[0], :], ds[0][:, cols], ROWS_T)
        for i in range(1, n):
            total += dot(o[o_rows[i], :], ds[i][:, cols], ROWS_T)
        held[:, cols] = total + prev_w[:, cols]
        w_copy(h).start()

    for i in range(n):
        stage[pl.ds(i * rows, rows), :] = dot(ds[i][...], w_out[...], COLS_T).astype(BF16)
        o_copy(i).start()
    for i in range(n):
        o_copy(i).wait()
    for h in range(tiles):
        w_copy(h).wait()


def last_proj(pieces, attn_out, w_out, prev, tile=512):
    n = len(pieces)
    tokens, cols = attn_out.shape
    width = w_out.shape[1]
    rows = pieces[0][0].shape[0]
    return pl.pallas_call(
        functools.partial(last_body, [(k, start) for _, k, start in pieces], tile),
        in_specs=[pl.BlockSpec(memory_space=pltpu.VMEM)] * (n + 3) + [ANY],
        out_specs=[ANY, ANY],
        out_shape=[jax.ShapeDtypeStruct((tokens, cols), BF16), jax.ShapeDtypeStruct((cols, width), F32)],
        scratch_shapes=[pltpu.VMEM((cols, width), F32), pltpu.VMEM((n * rows, cols), BF16),
                        pltpu.SemaphoreType.DMA((width // tile,)), pltpu.SemaphoreType.DMA((n,))],
        input_output_aliases={n + 3: 0},
        compiler_params=params(16 << 20),
        cost_estimate=pl.CostEstimate(flops=4 * n * rows * width * cols, bytes_accessed=8 << 20, transcendentals=0),
    )(*[a for a, _, _ in pieces], attn_out, w_out, prev[1], *hbm(prev[0]))


DX_PARTS = 2
DS_PIECES = (256, 256)


def solution(mesh):
    token_spec = P(("dp", "tp"), None)
    split_cols = P("dp", "tp")
    weight_cols = P(None, "tp")
    weight_rows = P("tp", None)

    def cross(a):
        return lax.ppermute(a, "tp", CROSS)

    def pair(a):
        return lax.ppermute(a, "tp", PAIR)

    def after(a, *others):
        return lax.optimization_barrier((a,) + others)[0]

    def body(x_norm, grad_y, u_gate, u_up, w_gate, w_up, w_down, x_in, gamma, grad_res, attn_out, w_out):
        gamma = gamma.reshape(1, -1)
        gy_far = cross(grad_y)
        gy_sib = pair(grad_y)
        x_far = cross(x_norm)
        x_sib = pair(x_norm)
        gap = spacer(gamma)

        args = (u_gate, u_up, w_down, w_gate, w_up)
        dg_near, du_near, gw_down, z_sib, p_own, p_sib = hidden(
            (OWN, SIB), (grad_y, gy_sib), 1, 1, *args, deps=(gap,), tile=256)
        p_pair = pair(p_sib)
        gy_far = after(gy_far, p_own)
        gy_diag = pair(gy_far)
        gap = spacer(p_own)
        dg_far, du_far, z_far, *parts = hidden((FAR, DIAG), (gy_far, gy_diag), DX_PARTS, 0, *args, deps=(gap,))
        p_far, p_diag = parts[:DX_PARTS], parts[DX_PARTS:]
        p_diag = [pair(p) for p in p_diag]
        sends = [add(a, b) for a, b in zip(p_far, p_diag)]
        recvs = [cross(p) for p in sends]
        x_far = after(x_far, sends[-1])
        x_diag = pair(x_far)
        gw_down = weight_grad([(z_sib, 0), (z_far, 0), (z_far, 1)], [(gy_sib, 0), (gy_far, 0), (gy_diag, 0)],
                              prev=gw_down, deps=(sends[-1],), tm=512)

        xs = [(x_norm, 0), (x_sib, 0), (x_far, 0), (x_diag, 0)]
        rest = [functools.partial(weight_grad, xs, [(dg_near, 0), (dg_near, 1), (dg_far, 0), (dg_far, 1)]),
                functools.partial(weight_grad, xs, [(du_near, 0), (du_near, 1), (du_far, 0), (du_far, 1)])]
        dx_rows = BLOCK // DX_PARTS
        whole, fars, places, grads, at, prev = None, [], [], [], 0, gw_down
        for c, n in enumerate(DS_PIECES):
            part = at // dx_rows
            piece, whole = norm_backward(at, n, p_own, p_pair, after(recvs[part], prev), at - part * dx_rows,
                                         x_in, grad_res, gamma, whole)
            fars.append(cross(piece))
            places.append(at)
            prev = piece
            if c < len(rest):
                prev = rest[c](deps=(piece,))
                grads.append(prev)
            at += n
        gw_gate, gw_up = grads
        sib = pair(whole)
        near = out_proj([(whole, OWN, 0), (sib, SIB, 0)], attn_out, w_out, None, deps=(gw_up,), tile=2048)
        pieces, prev = [], gw_up
        for c, at in enumerate(places):
            far = after(fars[c], prev)
            pieces += [(far, FAR, at), (pair(far), DIAG, at)]
            prev = near[1]
        grad_attn, gw_out = last_proj(pieces, attn_out, w_out, near)
        return whole, grad_attn, gw_gate, gw_up, gw_down, gw_out


    return jax.shard_map(
        body,
        mesh=mesh,
        in_specs=(token_spec, token_spec, split_cols, split_cols, weight_cols, weight_cols, weight_rows,
                  token_spec, P(None), token_spec, split_cols, weight_rows),
        out_specs=(token_spec, split_cols, split_cols, split_cols, token_spec, token_spec),
        check_vma=False,
    )
```

```python
import functools

import jax
import jax.numpy as jnp
from jax import lax
from jax.experimental import pallas as pl
from jax.experimental.pallas import tpu as pltpu
from jax.sharding import PartitionSpec as P


F32 = jnp.float32
BF16 = jnp.bfloat16
NORM_EPS = 1e-5
ROWS_T = (((0,), (0,)), ((), ()))
COLS_T = (((1,), (1,)), ((), ()))
ANY = pl.BlockSpec(memory_space=pl.ANY)
VMEM_LIMIT = 60 * 1024 * 1024
ALL_VMEM = 67043328
BLOCK = 512

CROSS = [(0, 2), (2, 0), (1, 3), (3, 1)]
PAIR = [(0, 1), (1, 0), (2, 3), (3, 2)]
OWN, SIB, FAR, DIAG = 0, 1, 2, 3


def dot(a, b, dims):
    return lax.dot_general(a, b, dims, preferred_element_type=F32)


def block_of(k):
    return lax.axis_index("tp") ^ k


def params(limit=VMEM_LIMIT):
    return pltpu.CompilerParams(vmem_limit_bytes=limit)


def hbm(*arrays):
    return [pltpu.with_memory_space_constraint(a, pltpu.HBM) for a in arrays]


def once(shape, index=None):
    return pl.BlockSpec(shape, index or (lambda *_: (0,) * len(shape)), pipeline_mode=pl.Buffered(1))


def hidden_body(n, tiles, parts, down, *refs):
    dys, ugs, uus = refs[:n], refs[n:2 * n], refs[2 * n:3 * n]
    wd, wg_all, wu_all = refs[3 * n:3 * n + 3]
    m = n * parts
    outs = refs[-(m + 8 + (down > 0) + (down < n)):-(m + 6)]
    dg, du = outs[:2]
    ps, (acc, held_g, held_u, wg, wu, sems) = refs[-(m + 6):-6], refs[-6:]
    step = pl.program_id(0)
    rows = dys[0].shape[0]
    piece = rows // parts

    def form(slot):
        total = None
        for i in range(n):
            span = pl.ds(i * rows, rows)
            grad_h = dot(dys[i][...], wd[...], COLS_T)
            gate = ugs[i][...].astype(F32)
            up = uus[i][...].astype(F32)
            sig = jax.nn.sigmoid(gate)
            act = gate * sig
            hidden_z = (act * up).astype(BF16)
            grad_up = (grad_h * act).astype(BF16)
            grad_gate = (grad_h * up * (sig * (1.0 + gate * (1.0 - sig)))).astype(BF16)
            du[span, :] = grad_up
            dg[span, :] = grad_gate
            held_u[slot, span, :] = grad_up
            held_g[slot, span, :] = grad_gate
            if i < down:
                more = dot(hidden_z, dys[i][...], ROWS_T)
                total = more if total is None else total + more
            else:
                outs[-1][pl.ds((i - down) * rows, rows), :] = hidden_z
        if down:
            outs[2][...] = total

    def fetch(k, slot):
        cols = pl.ds(pl.multiple_of(k * tile, tile), tile)
        return [pltpu.make_async_copy(wg_all.at[:, cols], wg.at[slot], sems.at[0, slot]),
                pltpu.make_async_copy(wu_all.at[:, cols], wu.at[slot], sems.at[1, slot])]

    def term(slot):
        return dot(held_g[slot], wg[slot], COLS_T) + dot(held_u[slot], wu[slot], COLS_T)

    tile = wd.shape[0]

    @pl.when(step == 0)
    def _():
        for c in fetch(0, 0):
            c.start()
        form(0)

    @pl.when((step > 0) & (step < tiles))
    def _():
        slot = lax.rem(step, 2)
        for c in fetch(step, slot):
            c.start()
        for c in fetch(step - 1, 1 - slot):
            c.wait()
        acc[...] = jnp.where(step == 1, 0.0, acc[...]) + term(1 - slot)
        form(slot)

    @pl.when(step == tiles)
    def _():
        last = (tiles - 1) % 2
        for c in fetch(tiles - 1, last):
            c.wait()
        total = acc[...] + term(last)
        for i in range(m):
            ps[i][...] = total[i * piece:(i + 1) * piece].astype(BF16)


def hidden(blocks, dys, parts, down, u_gate, u_up, w_down, w_gate, w_up, deps=(), tile=512):
    n = len(blocks)
    rows, width = dys[0].shape
    cols = w_down.shape[0]
    tiles = cols // tile
    now = lambda s: jnp.minimum(s, tiles - 1)
    u_specs = [pl.BlockSpec((rows, tile), functools.partial(lambda k, s: (block_of(k), now(s)), k)) for k in blocks]
    tile_out = pl.BlockSpec((n * rows, tile), lambda s: (0, now(s)))
    z_out = pl.BlockSpec(((n - down) * rows, tile), lambda s: (0, now(s)))
    w_now = pl.BlockSpec((tile, width), lambda s: (now(s), 0))
    wide = jax.ShapeDtypeStruct((n * rows, cols), BF16)
    piece = (rows // parts, width)
    return pl.pallas_call(
        functools.partial(hidden_body, n, tiles, parts, down),
        grid=(tiles + 1,),
        in_specs=[once((rows, width))] * n + u_specs + u_specs + [w_now, ANY, ANY] + [ANY] * len(deps),
        out_specs=[tile_out] * 2 + [w_now] * (down > 0) + [z_out] * (down < n) + [once(piece)] * (n * parts),
        out_shape=[wide] * 2 + [jax.ShapeDtypeStruct((cols, width), F32)] * (down > 0)
        + [jax.ShapeDtypeStruct(((n - down) * rows, cols), BF16)] * (down < n)
        + [jax.ShapeDtypeStruct(piece, BF16)] * (n * parts),
        scratch_shapes=[pltpu.VMEM((n * rows, width), F32)] + [pltpu.VMEM((2, n * rows, tile), BF16)] * 2
        + [pltpu.VMEM((2, width, tile), BF16)] * 2 + [pltpu.SemaphoreType.DMA((2, 2))],
        compiler_params=params(),
        cost_estimate=pl.CostEstimate(flops=(6 * n + 2 * down) * rows * width * cols, bytes_accessed=50 << 20,
                                      transcendentals=n * rows * cols),
    )(*dys, *hbm(*([u_gate] * n), *([u_up] * n), w_down, w_gate, w_up, *deps))


def grad_body(n, *refs):
    lefts, rights, out = refs[:n], refs[n:2 * n], refs[-1]
    total = dot(lefts[0][...], rights[0][...], ROWS_T)
    for a, b in zip(lefts[1:], rights[1:]):
        total += dot(a[...], b[...], ROWS_T)
    out[...] = total


def grad_more_body(n, *refs):
    lefts, rights, prev, out = refs[:n], refs[n:2 * n], refs[2 * n], refs[-1]
    total = prev[...]
    for a, b in zip(lefts, rights):
        total += dot(a[...], b[...], ROWS_T)
    out[...] = total


def weight_grad(lefts, rights, prev=None, deps=(), tm=256, limit=VMEM_LIMIT):
    n = len(lefts)
    m, cols = lefts[0][0].shape[1], rights[0][0].shape[1]
    l_specs = [pl.BlockSpec((BLOCK, tm), functools.partial(lambda b, i: (b, i), b)) for _, b in lefts]
    r_specs = [once((BLOCK, cols), functools.partial(lambda b, i: (b, 0), b)) for _, b in rights]
    out_spec = pl.BlockSpec((tm, cols), lambda i: (i, 0))
    more = [] if prev is None else [prev]
    return pl.pallas_call(
        functools.partial(grad_body if prev is None else grad_more_body, n),
        grid=(m // tm,),
        in_specs=l_specs + r_specs + [out_spec] * len(more) + [ANY] * len(deps),
        out_specs=out_spec,
        out_shape=jax.ShapeDtypeStruct((m, cols), F32),
        input_output_aliases={2 * n: 0} if more else {},
        compiler_params=params(limit),
        cost_estimate=pl.CostEstimate(flops=2 * n * BLOCK * m * cols, bytes_accessed=32 << 20, transcendentals=0),
    )(*hbm(*[a for a, _ in lefts], *[a for a, _ in rights], *more, *deps))


def spacer_body(*refs):
    refs[-1][...] = jnp.zeros_like(refs[-1])


def spacer(*deps):
    return pl.pallas_call(
        spacer_body,
        in_specs=[ANY] * len(deps),
        out_shape=jax.ShapeDtypeStruct((8, 128), F32),
        compiler_params=params(ALL_VMEM),
        cost_estimate=pl.CostEstimate(flops=1000, bytes_accessed=4096, transcendentals=0),
    )(*hbm(*deps))


def add_body(a, b, *refs):
    refs[-1][...] = (a[...].astype(F32) + b[...].astype(F32)).astype(BF16)


def add(a, b, tile=128):
    rows, width = a.shape
    spec = pl.BlockSpec((tile, width), lambda i: (i, 0))
    return pl.pallas_call(
        add_body,
        grid=(rows // tile,),
        in_specs=[spec, spec],
        out_specs=spec,
        out_shape=jax.ShapeDtypeStruct((rows, width), BF16),
        compiler_params=params(24 << 20),
        cost_estimate=pl.CostEstimate(flops=1000 * rows * width, bytes_accessed=6 * rows * width, transcendentals=0),
    )(*hbm(a), b)


def norm_body(p_own, p_pair, p_far, x_in, grad_res, gamma, *refs):
    piece, whole = refs[-2:]
    grad_x = (p_own[...].astype(F32) + p_pair[...].astype(F32) + p_far[...].astype(F32)).astype(BF16)
    xin = x_in[...].astype(F32)
    inv = lax.rsqrt(jnp.mean(xin * xin, axis=-1, keepdims=True) + NORM_EPS)
    scaled = grad_x.astype(F32) * gamma[...].astype(F32)
    proj = jnp.mean(scaled * xin, axis=-1, keepdims=True)
    res = (grad_res[...].astype(F32) + inv * (scaled - xin * (inv * inv) * proj)).astype(BF16)
    piece[...] = res
    whole[...] = res


def norm_backward(start, rows, p_own, p_pair, p_far, far_start, x_in, grad_res, gamma, prev, deps=(), tile=128):
    width = p_far.shape[1]
    first, far_first = start // tile, far_start // tile
    here = pl.BlockSpec((tile, width), lambda i: (first + i, 0))
    recv = pl.BlockSpec((tile, width), lambda i: (far_first + i, 0))
    part = pl.BlockSpec((tile, width), lambda i: (i, 0))
    extra = ([] if prev is None else [prev]) + list(deps)
    return pl.pallas_call(
        norm_body,
        grid=(rows // tile,),
        in_specs=[here, here, recv, here, here, once((1, width))] + [ANY] * len(extra),
        out_specs=[part, here],
        out_shape=[jax.ShapeDtypeStruct((rows, width), BF16), jax.ShapeDtypeStruct(p_own.shape, BF16)],
        input_output_aliases={} if prev is None else {6: 1},
        compiler_params=params(24 << 20),
        cost_estimate=pl.CostEstimate(flops=2000 * rows * width, bytes_accessed=14 * rows * width, transcendentals=0),
    )(*hbm(p_own, p_pair), p_far, *hbm(x_in, grad_res, gamma, *extra))


def proj_body(places, tile, more, *refs):
    n = len(places)
    ds, (o, w_out) = refs[:n], refs[n:n + 2]
    grad_o, grad_w, held, stage, sem_w, sem_o = refs[-6:]
    rows = ds[0].shape[0]
    tiles = w_out.shape[1] // tile
    o_rows = [pl.ds(pl.multiple_of(block_of(k) * BLOCK + start, rows), rows) for k, start in places]

    def w_copy(h):
        cols = pl.ds(pl.multiple_of(h * tile, tile), tile)
        return pltpu.make_async_copy(held.at[:, cols], grad_w.at[:, cols], sem_w.at[h])

    def o_copy(i):
        return pltpu.make_async_copy(stage.at[pl.ds(i * rows, rows), :], grad_o.at[o_rows[i], :], sem_o.at[i])

    @pl.loop(0, tiles)
    def _(h):
        cols = pl.ds(pl.multiple_of(h * tile, tile), tile)
        total = dot(o[o_rows[0], :], ds[0][:, cols], ROWS_T)
        for i in range(1, n):
            total += dot(o[o_rows[i], :], ds[i][:, cols], ROWS_T)
        held[:, cols] = total + refs[n + 2][:, cols] if more else total
        w_copy(h).start()

    for i in range(n):
        stage[pl.ds(i * rows, rows), :] = dot(ds[i][...], w_out[...], COLS_T).astype(BF16)
        o_copy(i).start()
    for i in range(n):
        o_copy(i).wait()
    for h in range(tiles):
        w_copy(h).wait()


def out_proj(pieces, attn_out, w_out, prev=None, deps=(), tile=1024):
    n = len(pieces)
    tokens, cols = attn_out.shape
    width = w_out.shape[1]
    rows = pieces[0][0].shape[0]
    vmem = pl.BlockSpec(memory_space=pltpu.VMEM)
    more = prev is not None
    return pl.pallas_call(
        functools.partial(proj_body, [(k, start) for _, k, start in pieces], tile, more),
        in_specs=[vmem] * (n + 2) + ([vmem, ANY] if more else []) + [ANY] * len(deps),
        out_specs=[ANY, ANY],
        out_shape=[jax.ShapeDtypeStruct((tokens, cols), BF16), jax.ShapeDtypeStruct((cols, width), F32)],
        scratch_shapes=[pltpu.VMEM((cols, width), F32), pltpu.VMEM((n * rows, cols), BF16),
                        pltpu.SemaphoreType.DMA((width // tile,)), pltpu.SemaphoreType.DMA((n,))],
        input_output_aliases={n + 3: 0} if more else {},
        compiler_params=params(16 << 20),
        cost_estimate=pl.CostEstimate(flops=4 * n * rows * width * cols, bytes_accessed=8 << 20, transcendentals=0),
    )(*[a for a, _, _ in pieces], attn_out, w_out, *([prev[1], *hbm(prev[0])] if more else []), *hbm(*deps))


DX_PARTS = 2
DS_PIECES = (256, 256)


def solution(mesh):
    token_spec = P(("dp", "tp"), None)
    split_cols = P("dp", "tp")
    weight_cols = P(None, "tp")
    weight_rows = P("tp", None)

    def cross(a):
        return lax.ppermute(a, "tp", CROSS)

    def pair(a):
        return lax.ppermute(a, "tp", PAIR)

    def after(a, *others):
        return lax.optimization_barrier((a,) + others)[0]

    def body(x_norm, grad_y, u_gate, u_up, w_gate, w_up, w_down, x_in, gamma, grad_res, attn_out, w_out):
        gamma = gamma.reshape(1, -1)
        gy_far = cross(grad_y)
        gy_sib = pair(grad_y)
        x_far = cross(x_norm)
        x_sib = pair(x_norm)
        gap = spacer(gamma)

        args = (u_gate, u_up, w_down, w_gate, w_up)
        dg_near, du_near, gw_down, z_sib, p_own, p_sib = hidden(
            (OWN, SIB), (grad_y, gy_sib), 1, 1, *args, deps=(gap,), tile=256)
        p_pair = pair(p_sib)
        gy_far = after(gy_far, p_own)
        gy_diag = pair(gy_far)
        gap = spacer(p_own)
        dg_far, du_far, z_far, *parts = hidden((FAR, DIAG), (gy_far, gy_diag), DX_PARTS, 0, *args, deps=(gap,))
        p_far, p_diag = parts[:DX_PARTS], parts[DX_PARTS:]
        p_diag = [pair(p) for p in p_diag]
        sends = [add(a, b) for a, b in zip(p_far, p_diag)]
        recvs = [cross(p) for p in sends]
        x_far = after(x_far, sends[-1])
        x_diag = pair(x_far)
        gw_down = weight_grad([(z_sib, 0), (z_far, 0), (z_far, 1)], [(gy_sib, 0), (gy_far, 0), (gy_diag, 0)],
                              prev=gw_down, deps=(sends[-1],), tm=512)

        xs = [(x_norm, 0), (x_sib, 0), (x_far, 0), (x_diag, 0)]
        rest = [functools.partial(weight_grad, xs, [(dg_near, 0), (dg_near, 1), (dg_far, 0), (dg_far, 1)]),
                functools.partial(weight_grad, xs, [(du_near, 0), (du_near, 1), (du_far, 0), (du_far, 1)], limit=48 << 20)]
        dx_rows = BLOCK // DX_PARTS
        whole, fars, places, grads, at, prev = None, [], [], [], 0, gw_down
        for c, n in enumerate(DS_PIECES):
            part = at // dx_rows
            piece, whole = norm_backward(at, n, p_own, p_pair, after(recvs[part], prev), at - part * dx_rows,
                                         x_in, grad_res, gamma, whole)
            fars.append(cross(piece))
            places.append(at)
            prev = piece
            if c < len(rest):
                prev = rest[c](deps=(piece,))
                grads.append(prev)
            at += n
        gw_gate, gw_up = grads
        sib = pair(whole)
        near = out_proj([(whole, OWN, 0), (sib, SIB, 0)], attn_out, w_out, deps=(gw_up,))
        pieces, prev = [], gw_up
        for c, at in enumerate(places):
            far = after(fars[c], prev)
            pieces += [(far, FAR, at), (pair(far), DIAG, at)]
            prev = near[1]
        grad_attn, gw_out = out_proj(pieces, attn_out, w_out, near)
        return whole, grad_attn, gw_gate, gw_up, gw_down, gw_out


    return jax.shard_map(
        body,
        mesh=mesh,
        in_specs=(token_spec, token_spec, split_cols, split_cols, weight_cols, weight_cols, weight_rows,
                  token_spec, P(None), token_spec, split_cols, weight_rows),
        out_specs=(token_spec, split_cols, split_cols, split_cols, token_spec, token_spec),
        check_vma=False,
    )
```

```python
import functools

import jax
import jax.numpy as jnp
from jax import lax
from jax.experimental import pallas as pl
from jax.experimental.pallas import tpu as pltpu
from jax.sharding import PartitionSpec as P


F32 = jnp.float32
BF16 = jnp.bfloat16
NORM_EPS = 1e-5
ROWS_T = (((0,), (0,)), ((), ()))
COLS_T = (((1,), (1,)), ((), ()))
ANY = pl.BlockSpec(memory_space=pl.ANY)
VMEM_LIMIT = 60 * 1024 * 1024
ALL_VMEM = 67043328
BLOCK = 512

CROSS = [(0, 2), (2, 0), (1, 3), (3, 1)]
PAIR = [(0, 1), (1, 0), (2, 3), (3, 2)]
OWN, SIB, FAR, DIAG = 0, 1, 2, 3


def dot(a, b, dims):
    return lax.dot_general(a, b, dims, preferred_element_type=F32)


def block_of(k):
    return lax.axis_index("tp") ^ k


def params(limit=VMEM_LIMIT):
    return pltpu.CompilerParams(vmem_limit_bytes=limit)


def hbm(*arrays):
    return [pltpu.with_memory_space_constraint(a, pltpu.HBM) for a in arrays]


def once(shape, index=None):
    return pl.BlockSpec(shape, index or (lambda *_: (0,) * len(shape)), pipeline_mode=pl.Buffered(1))


def hidden_body(n, tiles, parts, down, *refs):
    dy, dy_more, ugs, uus = refs[0], refs[1:n], refs[n:2 * n], refs[2 * n:3 * n]
    wd, wg_all, wu_all = refs[3 * n:3 * n + 3]
    m = n * parts
    outs = refs[-(m + 8 + n + (down > 0) + (down < n)):-(m + 6 + n)]
    dg, du = outs[:2]
    ps, (acc, held_g, held_u, wg, wu, sems, dy_sems) = refs[-(m + 6 + n):-(6 + n)], refs[-(6 + n):-n + 1][:6] + (refs[-1],)
    dys = (dy,) + refs[-n:-1]
    dy_copies = [pltpu.make_async_copy(a, b, dy_sems.at[k]) for k, (a, b) in enumerate(zip(dy_more, dys[1:]))]
    step = pl.program_id(0)
    rows = dy.shape[0]
    piece = rows // parts

    def form(slot, wait=False):
        total = None
        for i in range(n):
            if wait and i:
                dy_copies[i - 1].wait()
            span = pl.ds(i * rows, rows)
            grad_h = dot(dys[i][...], wd[...], COLS_T)
            gate = ugs[i][...].astype(F32)
            up = uus[i][...].astype(F32)
            sig = jax.nn.sigmoid(gate)
            act = gate * sig
            hidden_z = (act * up).astype(BF16)
            grad_up = (grad_h * act).astype(BF16)
            grad_gate = (grad_h * up * (sig * (1.0 + gate * (1.0 - sig)))).astype(BF16)
            du[span, :] = grad_up
            dg[span, :] = grad_gate
            held_u[slot, span, :] = grad_up
            held_g[slot, span, :] = grad_gate
            if i < down:
                more = dot(hidden_z, dys[i][...], ROWS_T)
                total = more if total is None else total + more
            else:
                outs[-1][pl.ds((i - down) * rows, rows), :] = hidden_z
        if down:
            outs[2][...] = total

    def fetch(k, slot):
        cols = pl.ds(pl.multiple_of(k * tile, tile), tile)
        return [pltpu.make_async_copy(wg_all.at[:, cols], wg.at[slot], sems.at[0, slot]),
                pltpu.make_async_copy(wu_all.at[:, cols], wu.at[slot], sems.at[1, slot])]

    def term(slot):
        return dot(held_g[slot], wg[slot], COLS_T) + dot(held_u[slot], wu[slot], COLS_T)

    tile = wd.shape[0]

    @pl.when(step == 0)
    def _():
        for c in dy_copies + fetch(0, 0):
            c.start()
        form(0, wait=True)

    @pl.when((step > 0) & (step < tiles))
    def _():
        slot = lax.rem(step, 2)
        for c in fetch(step, slot):
            c.start()
        for c in fetch(step - 1, 1 - slot):
            c.wait()
        acc[...] = jnp.where(step == 1, 0.0, acc[...]) + term(1 - slot)
        form(slot)

    @pl.when(step == tiles)
    def _():
        last = (tiles - 1) % 2
        for c in fetch(tiles - 1, last):
            c.wait()
        total = acc[...] + term(last)
        for i in range(m):
            ps[i][...] = total[i * piece:(i + 1) * piece].astype(BF16)


def hidden(blocks, dys, parts, down, u_gate, u_up, w_down, w_gate, w_up, deps=(), tile=512):
    n = len(blocks)
    rows, width = dys[0].shape
    cols = w_down.shape[0]
    tiles = cols // tile
    now = lambda s: jnp.minimum(s, tiles - 1)
    u_specs = [pl.BlockSpec((rows, tile), functools.partial(lambda k, s: (block_of(k), now(s)), k)) for k in blocks]
    tile_out = pl.BlockSpec((n * rows, tile), lambda s: (0, now(s)))
    z_out = pl.BlockSpec(((n - down) * rows, tile), lambda s: (0, now(s)))
    w_now = pl.BlockSpec((tile, width), lambda s: (now(s), 0))
    wide = jax.ShapeDtypeStruct((n * rows, cols), BF16)
    piece = (rows // parts, width)
    return pl.pallas_call(
        functools.partial(hidden_body, n, tiles, parts, down),
        grid=(tiles + 1,),
        in_specs=[once((rows, width))] + [ANY] * (n - 1) + u_specs + u_specs + [w_now, ANY, ANY] + [ANY] * len(deps),
        out_specs=[tile_out] * 2 + [w_now] * (down > 0) + [z_out] * (down < n) + [once(piece)] * (n * parts),
        out_shape=[wide] * 2 + [jax.ShapeDtypeStruct((cols, width), F32)] * (down > 0)
        + [jax.ShapeDtypeStruct(((n - down) * rows, cols), BF16)] * (down < n)
        + [jax.ShapeDtypeStruct(piece, BF16)] * (n * parts),
        scratch_shapes=[pltpu.VMEM((n * rows, width), F32)] + [pltpu.VMEM((2, n * rows, tile), BF16)] * 2
        + [pltpu.VMEM((2, width, tile), BF16)] * 2 + [pltpu.SemaphoreType.DMA((2, 2))]
        + [pltpu.VMEM((rows, width), BF16)] * (n - 1) + [pltpu.SemaphoreType.DMA((n - 1,))],
        compiler_params=params(),
        cost_estimate=pl.CostEstimate(flops=(6 * n + 2 * down) * rows * width * cols, bytes_accessed=50 << 20,
                                      transcendentals=n * rows * cols),
    )(*dys, *hbm(*([u_gate] * n), *([u_up] * n), w_down, w_gate, w_up, *deps))


def grad_body(n, *refs):
    lefts, rights, out = refs[:n], refs[n:2 * n], refs[-1]
    total = dot(lefts[0][...], rights[0][...], ROWS_T)
    for a, b in zip(lefts[1:], rights[1:]):
        total += dot(a[...], b[...], ROWS_T)
    out[...] = total


def grad_more_body(n, *refs):
    lefts, rights, prev, out = refs[:n], refs[n:2 * n], refs[2 * n], refs[-1]
    total = prev[...]
    for a, b in zip(lefts, rights):
        total += dot(a[...], b[...], ROWS_T)
    out[...] = total


def weight_grad(lefts, rights, prev=None, deps=(), tm=256, limit=VMEM_LIMIT):
    n = len(lefts)
    m, cols = lefts[0][0].shape[1], rights[0][0].shape[1]
    l_specs = [pl.BlockSpec((BLOCK, tm), functools.partial(lambda b, i: (b, i), b)) for _, b in lefts]
    r_specs = [once((BLOCK, cols), functools.partial(lambda b, i: (b, 0), b)) for _, b in rights]
    out_spec = pl.BlockSpec((tm, cols), lambda i: (i, 0))
    more = [] if prev is None else [prev]
    return pl.pallas_call(
        functools.partial(grad_body if prev is None else grad_more_body, n),
        grid=(m // tm,),
        in_specs=l_specs + r_specs + [out_spec] * len(more) + [ANY] * len(deps),
        out_specs=out_spec,
        out_shape=jax.ShapeDtypeStruct((m, cols), F32),
        input_output_aliases={2 * n: 0} if more else {},
        compiler_params=params(limit),
        cost_estimate=pl.CostEstimate(flops=2 * n * BLOCK * m * cols, bytes_accessed=32 << 20, transcendentals=0),
    )(*hbm(*[a for a, _ in lefts], *[a for a, _ in rights], *more, *deps))


def spacer_body(*refs):
    refs[-1][...] = jnp.zeros_like(refs[-1])


def spacer(*deps):
    return pl.pallas_call(
        spacer_body,
        in_specs=[ANY] * len(deps),
        out_shape=jax.ShapeDtypeStruct((8, 128), F32),
        compiler_params=params(ALL_VMEM),
        cost_estimate=pl.CostEstimate(flops=1000, bytes_accessed=4096, transcendentals=0),
    )(*hbm(*deps))


def add_body(a, b, *refs):
    refs[-1][...] = (a[...].astype(F32) + b[...].astype(F32)).astype(BF16)


def add(a, b, tile=128):
    rows, width = a.shape
    spec = pl.BlockSpec((tile, width), lambda i: (i, 0))
    return pl.pallas_call(
        add_body,
        grid=(rows // tile,),
        in_specs=[spec, spec],
        out_specs=spec,
        out_shape=jax.ShapeDtypeStruct((rows, width), BF16),
        compiler_params=params(24 << 20),
        cost_estimate=pl.CostEstimate(flops=1000 * rows * width, bytes_accessed=6 * rows * width, transcendentals=0),
    )(*hbm(a), b)


def norm_body(p_own, p_pair, p_far, x_in, grad_res, gamma, *refs):
    piece, whole = refs[-2:]
    grad_x = (p_own[...].astype(F32) + p_pair[...].astype(F32) + p_far[...].astype(F32)).astype(BF16)
    xin = x_in[...].astype(F32)
    inv = lax.rsqrt(jnp.mean(xin * xin, axis=-1, keepdims=True) + NORM_EPS)
    scaled = grad_x.astype(F32) * gamma[...].astype(F32)
    proj = jnp.mean(scaled * xin, axis=-1, keepdims=True)
    res = (grad_res[...].astype(F32) + inv * (scaled - xin * (inv * inv) * proj)).astype(BF16)
    piece[...] = res
    whole[...] = res


def norm_backward(start, rows, p_own, p_pair, p_far, far_start, x_in, grad_res, gamma, prev, deps=(), tile=128):
    width = p_far.shape[1]
    first, far_first = start // tile, far_start // tile
    here = pl.BlockSpec((tile, width), lambda i: (first + i, 0))
    recv = pl.BlockSpec((tile, width), lambda i: (far_first + i, 0))
    part = pl.BlockSpec((tile, width), lambda i: (i, 0))
    extra = ([] if prev is None else [prev]) + list(deps)
    return pl.pallas_call(
        norm_body,
        grid=(rows // tile,),
        in_specs=[here, here, recv, here, here, once((1, width))] + [ANY] * len(extra),
        out_specs=[part, here],
        out_shape=[jax.ShapeDtypeStruct((rows, width), BF16), jax.ShapeDtypeStruct(p_own.shape, BF16)],
        input_output_aliases={} if prev is None else {6: 1},
        compiler_params=params(24 << 20),
        cost_estimate=pl.CostEstimate(flops=2000 * rows * width, bytes_accessed=14 * rows * width, transcendentals=0),
    )(*hbm(p_own, p_pair), p_far, *hbm(x_in, grad_res, gamma), *extra)


def proj_body(places, tile, more, *refs):
    n = len(places)
    ds, (o, w_out) = refs[:n], refs[n:n + 2]
    grad_o, grad_w, stage, sem_o = refs[-4:] if not more else (refs[-6], refs[-5], refs[-3], refs[-1])
    held, sem_w = (refs[-4], refs[-2]) if more else (grad_w, None)
    rows = ds[0].shape[0]
    tiles = w_out.shape[1] // tile
    o_rows = [pl.ds(pl.multiple_of(block_of(k) * BLOCK + start, rows), rows) for k, start in places]

    def w_copy(h):
        cols = pl.ds(pl.multiple_of(h * tile, tile), tile)
        return pltpu.make_async_copy(held.at[:, cols], grad_w.at[:, cols], sem_w.at[h])

    def o_copy(i):
        return pltpu.make_async_copy(stage.at[pl.ds(i * rows, rows), :], grad_o.at[o_rows[i], :], sem_o.at[i])

    @pl.loop(0, tiles)
    def _(h):
        cols = pl.ds(pl.multiple_of(h * tile, tile), tile)
        total = dot(o[o_rows[0], :], ds[0][:, cols], ROWS_T)
        for i in range(1, n):
            total += dot(o[o_rows[i], :], ds[i][:, cols], ROWS_T)
        held[:, cols] = total + refs[n + 2][:, cols] if more else total
        if more:
            w_copy(h).start()

    for i in range(n):
        stage[pl.ds(i * rows, rows), :] = dot(ds[i][...], w_out[...], COLS_T).astype(BF16)
        o_copy(i).start()
    for i in range(n):
        o_copy(i).wait()
    for h in range(tiles if more else 0):
        w_copy(h).wait()


def out_proj(pieces, attn_out, w_out, prev=None, deps=(), tile=1024):
    n = len(pieces)
    tokens, cols = attn_out.shape
    width = w_out.shape[1]
    rows = pieces[0][0].shape[0]
    vmem = pl.BlockSpec(memory_space=pltpu.VMEM)
    more = prev is not None
    return pl.pallas_call(
        functools.partial(proj_body, [(k, start) for _, k, start in pieces], tile, more),
        in_specs=[vmem] * (n + 2) + ([vmem, ANY] if more else []) + [ANY] * len(deps),
        out_specs=[ANY, ANY if more else vmem],
        out_shape=[jax.ShapeDtypeStruct((tokens, cols), BF16), jax.ShapeDtypeStruct((cols, width), F32)],
        scratch_shapes=([pltpu.VMEM((cols, width), F32)] if more else []) + [pltpu.VMEM((n * rows, cols), BF16)]
        + ([pltpu.SemaphoreType.DMA((width // tile,))] if more else []) + [pltpu.SemaphoreType.DMA((n,))],
        input_output_aliases={n + 3: 0} if more else {},
        compiler_params=params(16 << 20),
        cost_estimate=pl.CostEstimate(flops=4 * n * rows * width * cols, bytes_accessed=8 << 20, transcendentals=0),
    )(*[a for a, _, _ in pieces], attn_out, w_out, *([prev[1], *hbm(prev[0])] if more else []), *hbm(*deps))


DX_PARTS = 2
DS_PIECES = (256, 256)


def solution(mesh):
    token_spec = P(("dp", "tp"), None)
    split_cols = P("dp", "tp")
    weight_cols = P(None, "tp")
    weight_rows = P("tp", None)

    def cross(a):
        return lax.ppermute(a, "tp", CROSS)

    def pair(a):
        return lax.ppermute(a, "tp", PAIR)

    def after(a, *others):
        return lax.optimization_barrier((a,) + others)[0]

    def body(x_norm, grad_y, u_gate, u_up, w_gate, w_up, w_down, x_in, gamma, grad_res, attn_out, w_out):
        gamma = gamma.reshape(1, -1)
        gy_far = cross(grad_y)
        gy_sib = pair(grad_y)
        x_far = cross(x_norm)
        x_sib = pair(x_norm)
        gap = spacer(gamma)

        args = (u_gate, u_up, w_down, w_gate, w_up)
        dg_near, du_near, gw_down, z_sib, p_own, p_sib = hidden(
            (OWN, SIB), (grad_y, gy_sib), 1, 1, *args, deps=(gap,), tile=256)
        p_pair = pair(p_sib)
        gy_far = after(gy_far, p_own)
        gy_diag = pair(gy_far)
        gap = spacer(p_own)
        dg_far, du_far, z_far, *parts = hidden((FAR, DIAG), (gy_far, gy_diag), DX_PARTS, 0, *args, deps=(gap,))
        p_far, p_diag = parts[:DX_PARTS], parts[DX_PARTS:]
        p_diag = [pair(p) for p in p_diag]
        sends = [add(a, b) for a, b in zip(p_far, p_diag)]
        recvs = [cross(p) for p in sends]
        x_far = after(x_far, sends[-1])
        x_diag = pair(x_far)
        gw_down = weight_grad([(z_sib, 0), (z_far, 0), (z_far, 1)], [(gy_sib, 0), (gy_far, 0), (gy_diag, 0)],
                              prev=gw_down, tm=512)

        xs = [(x_norm, 0), (x_sib, 0), (x_far, 0), (x_diag, 0)]
        rest = [functools.partial(weight_grad, xs, [(dg_near, 0), (dg_near, 1), (dg_far, 0), (dg_far, 1)]),
                functools.partial(weight_grad, xs, [(du_near, 0), (du_near, 1), (du_far, 0), (du_far, 1)], limit=48 << 20)]
        dx_rows = BLOCK // DX_PARTS
        whole, fars, places, grads, at, prev = None, [], [], [], 0, gw_down
        for c, n in enumerate(DS_PIECES):
            part = at // dx_rows
            piece, whole = norm_backward(at, n, p_own, p_pair, after(recvs[part], prev), at - part * dx_rows,
                                         x_in, grad_res, gamma, whole)
            fars.append(cross(piece))
            places.append(at)
            prev = piece
            if c < len(rest):
                prev = rest[c]()
                grads.append(prev)
            at += n
        gw_gate, gw_up = grads
        sib = pair(whole)
        near = out_proj([(whole, OWN, 0), (sib, SIB, 0)], attn_out, w_out, deps=(gw_up,))
        pieces, prev = [], gw_up
        for c, at in enumerate(places):
            far = after(fars[c], prev)
            pieces += [(far, FAR, at), (pair(far), DIAG, at)]
            prev = near[1]
        grad_attn, gw_out = out_proj(pieces, attn_out, w_out, near)
        return whole, grad_attn, gw_gate, gw_up, gw_down, gw_out


    return jax.shard_map(
        body,
        mesh=mesh,
        in_specs=(token_spec, token_spec, split_cols, split_cols, weight_cols, weight_cols, weight_rows,
                  token_spec, P(None), token_spec, split_cols, weight_rows),
        out_specs=(token_spec, split_cols, split_cols, split_cols, token_spec, token_spec),
        check_vma=False,
    )
```

```python
import functools

import jax
import jax.numpy as jnp
from jax import lax
from jax.experimental import pallas as pl
from jax.experimental.pallas import tpu as pltpu
from jax.sharding import PartitionSpec as P


F32 = jnp.float32
BF16 = jnp.bfloat16
NORM_EPS = 1e-5
ROWS_T = (((0,), (0,)), ((), ()))
COLS_T = (((1,), (1,)), ((), ()))
ANY = pl.BlockSpec(memory_space=pl.ANY)
VMEM_LIMIT = 60 * 1024 * 1024
ALL_VMEM = 67043328
BLOCK = 512

CROSS = [(0, 2), (2, 0), (1, 3), (3, 1)]
PAIR = [(0, 1), (1, 0), (2, 3), (3, 2)]
OWN, SIB, FAR, DIAG = 0, 1, 2, 3


def dot(a, b, dims):
    return lax.dot_general(a, b, dims, preferred_element_type=F32)


def block_of(k):
    return lax.axis_index("tp") ^ k


def params(limit=VMEM_LIMIT):
    return pltpu.CompilerParams(vmem_limit_bytes=limit)


def hbm(*arrays):
    return [pltpu.with_memory_space_constraint(a, pltpu.HBM) for a in arrays]


def once(shape, index=None):
    return pl.BlockSpec(shape, index or (lambda *_: (0,) * len(shape)), pipeline_mode=pl.Buffered(1))


def hidden_body(n, tiles, parts, down, *refs):
    dy, dy_more, ugs, uus = refs[0], refs[1:n], refs[n:2 * n], refs[2 * n:3 * n]
    wd, wg_all, wu_all = refs[3 * n:3 * n + 3]
    m = n * parts
    outs = refs[-(m + 8 + n + (down > 0) + (down < n)):-(m + 6 + n)]
    dg, du = outs[:2]
    ps, (acc, held_g, held_u, wg, wu, sems, dy_sems) = refs[-(m + 6 + n):-(6 + n)], refs[-(6 + n):-n + 1][:6] + (refs[-1],)
    dys = (dy,) + refs[-n:-1]
    dy_copies = [pltpu.make_async_copy(a, b, dy_sems.at[k]) for k, (a, b) in enumerate(zip(dy_more, dys[1:]))]
    step = pl.program_id(0)
    rows = dy.shape[0]
    piece = rows // parts

    def form(slot, wait=False):
        total = None
        for i in range(n):
            if wait and i:
                dy_copies[i - 1].wait()
            span = pl.ds(i * rows, rows)
            grad_h = dot(dys[i][...], wd[...], COLS_T)
            gate = ugs[i][...].astype(F32)
            up = uus[i][...].astype(F32)
            sig = jax.nn.sigmoid(gate)
            act = gate * sig
            hidden_z = (act * up).astype(BF16)
            grad_up = (grad_h * act).astype(BF16)
            grad_gate = (grad_h * up * (sig * (1.0 + gate * (1.0 - sig)))).astype(BF16)
            du[span, :] = grad_up
            dg[span, :] = grad_gate
            held_u[slot, span, :] = grad_up
            held_g[slot, span, :] = grad_gate
            if i < down:
                more = dot(hidden_z, dys[i][...], ROWS_T)
                total = more if total is None else total + more
            else:
                outs[-1][pl.ds((i - down) * rows, rows), :] = hidden_z
        if down:
            outs[2][...] = total

    def fetch(k, slot):
        cols = pl.ds(pl.multiple_of(k * tile, tile), tile)
        return [pltpu.make_async_copy(wg_all.at[:, cols], wg.at[slot], sems.at[0, slot]),
                pltpu.make_async_copy(wu_all.at[:, cols], wu.at[slot], sems.at[1, slot])]

    def term(slot):
        return dot(held_g[slot], wg[slot], COLS_T) + dot(held_u[slot], wu[slot], COLS_T)

    tile = wd.shape[0]

    @pl.when(step == 0)
    def _():
        for c in dy_copies + fetch(0, 0):
            c.start()
        form(0, wait=True)

    @pl.when((step > 0) & (step < tiles))
    def _():
        slot = lax.rem(step, 2)
        for c in fetch(step, slot):
            c.start()
        for c in fetch(step - 1, 1 - slot):
            c.wait()
        acc[...] = jnp.where(step == 1, 0.0, acc[...]) + term(1 - slot)
        form(slot)

    @pl.when(step == tiles)
    def _():
        last = (tiles - 1) % 2
        for c in fetch(tiles - 1, last):
            c.wait()
        total = acc[...] + term(last)
        for i in range(m):
            ps[i][...] = total[i * piece:(i + 1) * piece].astype(BF16)


def hidden(blocks, dys, parts, down, u_gate, u_up, w_down, w_gate, w_up, deps=(), tile=512):
    n = len(blocks)
    rows, width = dys[0].shape
    cols = w_down.shape[0]
    tiles = cols // tile
    now = lambda s: jnp.minimum(s, tiles - 1)
    u_specs = [pl.BlockSpec((rows, tile), functools.partial(lambda k, s: (block_of(k), now(s)), k)) for k in blocks]
    tile_out = pl.BlockSpec((n * rows, tile), lambda s: (0, now(s)))
    z_out = pl.BlockSpec(((n - down) * rows, tile), lambda s: (0, now(s)))
    w_now = pl.BlockSpec((tile, width), lambda s: (now(s), 0))
    wide = jax.ShapeDtypeStruct((n * rows, cols), BF16)
    piece = (rows // parts, width)
    return pl.pallas_call(
        functools.partial(hidden_body, n, tiles, parts, down),
        grid=(tiles + 1,),
        in_specs=[once((rows, width))] + [ANY] * (n - 1) + u_specs + u_specs + [w_now, ANY, ANY] + [ANY] * len(deps),
        out_specs=[tile_out] * 2 + [w_now] * (down > 0) + [z_out] * (down < n) + [once(piece)] * (n * parts),
        out_shape=[wide] * 2 + [jax.ShapeDtypeStruct((cols, width), F32)] * (down > 0)
        + [jax.ShapeDtypeStruct(((n - down) * rows, cols), BF16)] * (down < n)
        + [jax.ShapeDtypeStruct(piece, BF16)] * (n * parts),
        scratch_shapes=[pltpu.VMEM((n * rows, width), F32)] + [pltpu.VMEM((2, n * rows, tile), BF16)] * 2
        + [pltpu.VMEM((2, width, tile), BF16)] * 2 + [pltpu.SemaphoreType.DMA((2, 2))]
        + [pltpu.VMEM((rows, width), BF16)] * (n - 1) + [pltpu.SemaphoreType.DMA((n - 1,))],
        compiler_params=params(),
        cost_estimate=pl.CostEstimate(flops=(6 * n + 2 * down) * rows * width * cols, bytes_accessed=50 << 20,
                                      transcendentals=n * rows * cols),
    )(*dys, *hbm(*([u_gate] * n), *([u_up] * n), w_down, w_gate, w_up, *deps))


def grad_body(n, *refs):
    lefts, rights, out = refs[:n], refs[n:2 * n], refs[-1]
    total = dot(lefts[0][...], rights[0][...], ROWS_T)
    for a, b in zip(lefts[1:], rights[1:]):
        total += dot(a[...], b[...], ROWS_T)
    out[...] = total


def grad_more_body(n, *refs):
    lefts, rights, prev, out = refs[:n], refs[n:2 * n], refs[2 * n], refs[-1]
    total = prev[...]
    for a, b in zip(lefts, rights):
        total += dot(a[...], b[...], ROWS_T)
    out[...] = total


def weight_grad(lefts, rights, prev=None, deps=(), tm=256, limit=VMEM_LIMIT):
    n = len(lefts)
    m, cols = lefts[0][0].shape[1], rights[0][0].shape[1]
    l_specs = [pl.BlockSpec((BLOCK, tm), functools.partial(lambda b, i: (b, i), b)) for _, b in lefts]
    r_specs = [once((BLOCK, cols), functools.partial(lambda b, i: (b, 0), b)) for _, b in rights]
    out_spec = pl.BlockSpec((tm, cols), lambda i: (i, 0))
    more = [] if prev is None else [prev]
    return pl.pallas_call(
        functools.partial(grad_body if prev is None else grad_more_body, n),
        grid=(m // tm,),
        in_specs=l_specs + r_specs + [out_spec] * len(more) + [ANY] * len(deps),
        out_specs=out_spec,
        out_shape=jax.ShapeDtypeStruct((m, cols), F32),
        input_output_aliases={2 * n: 0} if more else {},
        compiler_params=params(limit),
        cost_estimate=pl.CostEstimate(flops=2 * n * BLOCK * m * cols, bytes_accessed=32 << 20, transcendentals=0),
    )(*hbm(*[a for a, _ in lefts], *[a for a, _ in rights], *more, *deps))


def spacer_body(*refs):
    refs[-1][...] = jnp.zeros_like(refs[-1])


def spacer(*deps):
    return pl.pallas_call(
        spacer_body,
        in_specs=[ANY] * len(deps),
        out_shape=jax.ShapeDtypeStruct((8, 128), F32),
        compiler_params=params(ALL_VMEM),
        cost_estimate=pl.CostEstimate(flops=1000, bytes_accessed=4096, transcendentals=0),
    )(*hbm(*deps))


def add_body(a, b, *refs):
    refs[-1][...] = (a[...].astype(F32) + b[...].astype(F32)).astype(BF16)


def add(a, b, tile=128):
    rows, width = a.shape
    spec = pl.BlockSpec((tile, width), lambda i: (i, 0))
    return pl.pallas_call(
        add_body,
        grid=(rows // tile,),
        in_specs=[spec, spec],
        out_specs=spec,
        out_shape=jax.ShapeDtypeStruct((rows, width), BF16),
        compiler_params=params(24 << 20),
        cost_estimate=pl.CostEstimate(flops=1000 * rows * width, bytes_accessed=6 * rows * width, transcendentals=0),
    )(*hbm(a), b)


def norm_body(p_own, p_pair, p_far, x_in, grad_res, gamma, *refs):
    piece, whole = refs[-2:]
    grad_x = (p_own[...].astype(F32) + p_pair[...].astype(F32) + p_far[...].astype(F32)).astype(BF16)
    xin = x_in[...].astype(F32)
    inv = lax.rsqrt(jnp.mean(xin * xin, axis=-1, keepdims=True) + NORM_EPS)
    scaled = grad_x.astype(F32) * gamma[...].astype(F32)
    proj = jnp.mean(scaled * xin, axis=-1, keepdims=True)
    res = (grad_res[...].astype(F32) + inv * (scaled - xin * (inv * inv) * proj)).astype(BF16)
    piece[...] = res
    whole[...] = res


def norm_backward(start, rows, p_own, p_pair, p_far, far_start, x_in, grad_res, gamma, prev, deps=(), tile=128):
    width = p_far.shape[1]
    first, far_first = start // tile, far_start // tile
    here = pl.BlockSpec((tile, width), lambda i: (first + i, 0))
    recv = pl.BlockSpec((tile, width), lambda i: (far_first + i, 0))
    part = pl.BlockSpec((tile, width), lambda i: (i, 0))
    extra = ([] if prev is None else [prev]) + list(deps)
    return pl.pallas_call(
        norm_body,
        grid=(rows // tile,),
        in_specs=[here, here, recv, here, here, once((1, width))] + [ANY] * len(extra),
        out_specs=[part, here],
        out_shape=[jax.ShapeDtypeStruct((rows, width), BF16), jax.ShapeDtypeStruct(p_own.shape, BF16)],
        input_output_aliases={} if prev is None else {6: 1},
        compiler_params=params(24 << 20),
        cost_estimate=pl.CostEstimate(flops=2000 * rows * width, bytes_accessed=14 * rows * width, transcendentals=0),
    )(*hbm(p_own, p_pair), p_far, *hbm(x_in, grad_res, gamma), *extra)


def proj_body(places, tile, more, keep, *refs):
    n = len(places)
    ds, (o, w_out) = refs[:n], refs[n:n + 2]
    grad_o, grad_w, stage, sem_o = refs[-4:] if keep else (refs[-6], refs[-5], refs[-3], refs[-1])
    held, sem_w = (grad_w, None) if keep else (refs[-4], refs[-2])
    rows = ds[0].shape[0]
    tiles = w_out.shape[1] // tile
    o_rows = [pl.ds(pl.multiple_of(block_of(k) * BLOCK + start, rows), rows) for k, start in places]

    def w_copy(h):
        cols = pl.ds(pl.multiple_of(h * tile, tile), tile)
        return pltpu.make_async_copy(held.at[:, cols], grad_w.at[:, cols], sem_w.at[h])

    def o_copy(i):
        return pltpu.make_async_copy(stage.at[pl.ds(i * rows, rows), :], grad_o.at[o_rows[i], :], sem_o.at[i])

    @pl.loop(0, tiles)
    def _(h):
        cols = pl.ds(pl.multiple_of(h * tile, tile), tile)
        total = dot(o[o_rows[0], :], ds[0][:, cols], ROWS_T)
        for i in range(1, n):
            total += dot(o[o_rows[i], :], ds[i][:, cols], ROWS_T)
        held[:, cols] = total + refs[n + 2][:, cols] if more else total
        if not keep:
            w_copy(h).start()

    for i in range(n):
        stage[pl.ds(i * rows, rows), :] = dot(ds[i][...], w_out[...], COLS_T).astype(BF16)
        o_copy(i).start()
    for i in range(n):
        o_copy(i).wait()
    for h in range(0 if keep else tiles):
        w_copy(h).wait()


def out_proj(pieces, attn_out, w_out, prev=None, keep=False, deps=(), tile=1024):
    n = len(pieces)
    tokens, cols = attn_out.shape
    width = w_out.shape[1]
    rows = pieces[0][0].shape[0]
    vmem = pl.BlockSpec(memory_space=pltpu.VMEM)
    more = prev is not None
    return pl.pallas_call(
        functools.partial(proj_body, [(k, start) for _, k, start in pieces], tile, more, keep),
        in_specs=[vmem] * (n + 2) + ([vmem, ANY] if more else []) + [ANY] * len(deps),
        out_specs=[ANY, vmem if keep else ANY],
        out_shape=[jax.ShapeDtypeStruct((tokens, cols), BF16), jax.ShapeDtypeStruct((cols, width), F32)],
        scratch_shapes=([] if keep else [pltpu.VMEM((cols, width), F32)]) + [pltpu.VMEM((n * rows, cols), BF16)]
        + ([] if keep else [pltpu.SemaphoreType.DMA((width // tile,))]) + [pltpu.SemaphoreType.DMA((n,))],
        input_output_aliases={n + 3: 0} if more else {},
        compiler_params=params(16 << 20),
        cost_estimate=pl.CostEstimate(flops=4 * n * rows * width * cols, bytes_accessed=8 << 20, transcendentals=0),
    )(*[a for a, _, _ in pieces], attn_out, w_out, *([prev[1], *hbm(prev[0])] if more else []), *hbm(*deps))


DX_PARTS = 2
DS_PIECES = (256, 256)


def solution(mesh):
    token_spec = P(("dp", "tp"), None)
    split_cols = P("dp", "tp")
    weight_cols = P(None, "tp")
    weight_rows = P("tp", None)

    def cross(a):
        return lax.ppermute(a, "tp", CROSS)

    def pair(a):
        return lax.ppermute(a, "tp", PAIR)

    def after(a, *others):
        return lax.optimization_barrier((a,) + others)[0]

    def body(x_norm, grad_y, u_gate, u_up, w_gate, w_up, w_down, x_in, gamma, grad_res, attn_out, w_out):
        gamma = gamma.reshape(1, -1)
        gy_far = cross(grad_y)
        gy_sib = pair(grad_y)
        x_far = cross(x_norm)
        x_sib = pair(x_norm)
        gap = spacer(gamma)

        args = (u_gate, u_up, w_down, w_gate, w_up)
        dg_near, du_near, gw_down, z_sib, p_own, p_sib = hidden(
            (OWN, SIB), (grad_y, gy_sib), 1, 1, *args, deps=(gap,), tile=256)
        p_pair = pair(p_sib)
        gy_far = after(gy_far, p_own)
        gy_diag = pair(gy_far)
        gap = spacer(p_own)
        dg_far, du_far, z_far, *parts = hidden((FAR, DIAG), (gy_far, gy_diag), DX_PARTS, 0, *args, deps=(gap,))
        p_far, p_diag = parts[:DX_PARTS], parts[DX_PARTS:]
        p_diag = [pair(p) for p in p_diag]
        sends = [add(a, b) for a, b in zip(p_far, p_diag)]
        recvs = [cross(p) for p in sends]
        x_far = after(x_far, sends[-1])
        x_diag = pair(x_far)
        gw_down = weight_grad([(z_sib, 0), (z_far, 0), (z_far, 1)], [(gy_sib, 0), (gy_far, 0), (gy_diag, 0)],
                              prev=gw_down, tm=512)

        xs = [(x_norm, 0), (x_sib, 0), (x_far, 0), (x_diag, 0)]
        rest = [functools.partial(weight_grad, xs, [(dg_near, 0), (dg_near, 1), (dg_far, 0), (dg_far, 1)]),
                functools.partial(weight_grad, xs, [(du_near, 0), (du_near, 1), (du_far, 0), (du_far, 1)], limit=48 << 20)]
        dx_rows = BLOCK // DX_PARTS
        whole, fars, places, grads, at, prev = None, [], [], [], 0, gw_down
        for c, n in enumerate(DS_PIECES):
            part = at // dx_rows
            piece, whole = norm_backward(at, n, p_own, p_pair, after(recvs[part], prev), at - part * dx_rows,
                                         x_in, grad_res, gamma, whole)
            fars.append(cross(piece))
            places.append(at)
            prev = piece
            if c < len(rest):
                prev = rest[c]()
                grads.append(prev)
            at += n
        gw_gate, gw_up = grads
        sib = pair(whole)
        near = out_proj([(whole, OWN, 0), (sib, SIB, 0)], attn_out, w_out, keep=True, deps=(gw_up,))
        pieces, prev = [], gw_up
        for c, at in enumerate(places):
            far = after(fars[c], prev)
            pieces += [(far, FAR, at), (pair(far), DIAG, at)]
            prev = near[1]
        most = out_proj(pieces[:-1], attn_out, w_out, near, keep=True)
        grad_attn, gw_out = out_proj(pieces[-1:], attn_out, w_out, most)
        return whole, grad_attn, gw_gate, gw_up, gw_down, gw_out


    return jax.shard_map(
        body,
        mesh=mesh,
        in_specs=(token_spec, token_spec, split_cols, split_cols, weight_cols, weight_cols, weight_rows,
                  token_spec, P(None), token_spec, split_cols, weight_rows),
        out_specs=(token_spec, split_cols, split_cols, split_cols, token_spec, token_spec),
        check_vma=False,
    )
```
